32 devices in a mesh: groups: 2 (over y), expert: 8 (over z, x), dp: 2 (over core).
Axes of the slice: x: 2, y: 2, z: 4, core: 2. Of those that a mesh axis runs over, the one named last changes fastest.
Arguments:
- tokens: bfloat16 [2048, 2560], P(('groups', 'expert', 'dp')), parts along dimension 0, may hold values from -6 to 6
- group_ids: int32 [2048, 2], P(('groups', 'expert', 'dp')), parts along dimension 0, may hold values from 0 to 1, as said below
- expert_ids: int32 [2048, 6], P(('groups', 'expert', 'dp')), parts along dimension 0, may hold values from 0 to 5, as said below
- gate_weights: bfloat16 [2048, 6], P(('groups', 'expert', 'dp')), parts along dimension 0, may hold values from 0.019897461 to 0.59765625
- gate_proj: bfloat16 [8, 2560, 576], P('expert', 'dp'), may hold values from -0.125 to 0.125
- up_proj: bfloat16 [8, 2560, 576], P('expert', 'dp'), may hold values from -0.125 to 0.125
- down_proj: bfloat16 [8, 2560, 576], P('expert', 'dp'), may hold values from -0.21875 to 0.21875
Outputs:
- moe_out: bfloat16 [2048, 2560], P(('groups', 'expert', 'dp')), parts along dimension 0
The draws below stay inside these ranges and needn't reach their ends.
There are 2 independent parts, one for each index of `groups`. The reference program is written for one: setup_inputs(seed, part) draws one part's arguments, and reference() takes and returns one part's arrays. A program takes and returns all parts, laid end to end along the dimension named above; an argument that names none is the same for every part. Nothing has to cross between parts.
Inputs may be any that keep to these rules, and one draw needn't show every extreme that they name: `group_ids`: each row holds 2 distinct expert groups. `expert_ids`: each row holds 6 distinct experts, each of them in one of the row's groups; expert e belongs to group e // 3.
All inputs are finite; a program needn't handle non-finite values.
Results may differ from the reference program's by a relative error of at most 0.0078.
Values may be sent and summed in bfloat16 or wider, within the bound.
A program may use at most 128 MiB of HBM per device.

```python
import math
import jax
import jax.numpy as jnp
from jax import lax

D = 2560
HID = 768
GROUP_EXP = 3
SPAN = 4
TOPK = 6
TOK_DEV = 64
CAP = 8
GROUPS = 2
HSLICE = 192
ROUTE_GROUPS = 2
TOKENS = 1024
N_EXPERT = 8


def route_draw(key):
    base = jax.random.fold_in(key, 7)
    key_bias, key_noise, key_pick = jax.random.split(base, 3)
    bias = jax.random.randint(key_bias, (GROUPS,), 0, 400)
    noise = jax.random.randint(key_noise, (TOKENS, GROUPS), 0, 1000)
    scores = (bias[None, :] + noise) * GROUPS + jnp.arange(GROUPS, dtype=jnp.int32)[None, :]
    unused, chosen = lax.top_k(scores, ROUTE_GROUPS)
    chosen = chosen.astype(jnp.int32)
    width_cand = ROUTE_GROUPS * GROUP_EXP
    candidates = (chosen[:, :, None] * GROUP_EXP + jnp.arange(GROUP_EXP, dtype=jnp.int32)).reshape(TOKENS, width_cand)
    pick_scores = jax.random.randint(key_pick, (TOKENS, width_cand), 0, 1000) * width_cand + jnp.arange(width_cand, dtype=jnp.int32)[None, :]
    unused_two, picked = lax.top_k(pick_scores, TOPK)
    experts = jnp.take_along_axis(candidates, picked.astype(jnp.int32), axis=1)
    return (chosen, experts.astype(jnp.int32))


def draw_group_ids(key, part):
    return route_draw(key)[0]


def draw_expert_ids(key, part):
    return route_draw(key)[1]


def levels(key, dims, cuts, least, high):
    level = 1.0
    for dim, parts in cuts:
        steps = jax.random.uniform(jax.random.fold_in(jax.random.fold_in(key, 6), dim), (parts,), jnp.float32, least / len(cuts), high / len(cuts))
        level = level * jnp.repeat(jnp.exp(steps), dims[dim] // parts).reshape((-1,) + (1,) * (len(dims) - 1 - dim))
    return level


def normal_values(own_key, dims, deviation, reach, cuts=(), kind=jnp.bfloat16):
    values = deviation * jax.random.normal(own_key, dims, jnp.float32)
    if cuts:
        values = values * levels(own_key, dims, cuts, -0.22, 0.18)
    return jnp.clip(values, -reach, reach).astype(kind)


def setup_inputs(seed: int = 0, part: int = 0) -> dict:
    streams_of = jax.random.split(jax.random.key(seed), 8)
    part_splits = jax.random.split(jax.random.fold_in(streams_of[7], part), 8)
    return {
        "tokens": normal_values(part_splits[0], (TOKENS, D), 1.0, 6.0, ((0, 16),)),
        "group_ids": draw_group_ids(jax.random.fold_in(jax.random.fold_in(streams_of[7], part), 71), part),
        "expert_ids": draw_expert_ids(jax.random.fold_in(jax.random.fold_in(streams_of[7], part), 71), part),
        "gate_weights": jnp.clip(jnp.exp(math.log(0.59765625) - 3.4024236 * jax.random.uniform(part_splits[3], (TOKENS, TOPK), jnp.float32) ** levels(part_splits[3], (TOKENS, TOPK), ((0, 16),), -0.2, 0.2)), 0.019897461, 0.59765625).astype(jnp.bfloat16),
        "gate_proj": normal_values(streams_of[4], (N_EXPERT, D, GROUP_EXP * HSLICE), D ** -0.5, 0.125, ((0, 8), (1, 2))),
        "up_proj": normal_values(streams_of[5], (N_EXPERT, D, GROUP_EXP * HSLICE), D ** -0.5, 0.125, ((0, 8), (1, 2))),
        "down_proj": normal_values(streams_of[6], (N_EXPERT, D, GROUP_EXP * HSLICE), HID ** -0.5, 0.21875, ((0, 8), (1, 2))),
    }


def reference(tokens, group_ids, expert_ids, gate_weights, gate_proj, up_proj, down_proj):
    shards = TOKENS // TOK_DEV
    inputs = tokens.astype(jnp.float32).reshape(shards, TOK_DEV, D)
    chosen = group_ids.reshape(shards, TOK_DEV, ROUTE_GROUPS)
    experts = expert_ids.reshape(shards, TOK_DEV, TOPK)
    weights = gate_weights.astype(jnp.float32).reshape(shards, TOK_DEV, TOPK)
    group_iota = jnp.arange(GROUPS, dtype=jnp.int32)
    member = jnp.sum((chosen[..., None] == group_iota).astype(jnp.int32), axis=2)
    rank = jnp.cumsum(member, axis=1) - member
    kept = member * (rank < CAP).astype(jnp.int32)
    slot_iota = jnp.arange(CAP, dtype=jnp.int32)
    width_cols = GROUP_EXP * HSLICE

    def one_group(total, group):
        select = (kept[:, :, group][..., None] * (rank[:, :, group][..., None] == slot_iota).astype(jnp.int32)).astype(jnp.float32)
        local_experts = group * GROUP_EXP + jnp.arange(GROUP_EXP, dtype=jnp.int32)
        factor = jnp.sum(weights[..., None] * (experts[..., None] == local_experts).astype(jnp.float32), axis=2)
        rows = jnp.einsum('stc,std->scd', select, inputs).reshape(shards * CAP, D)
        row_factor = jnp.einsum('stc,stk->sck', select, factor).reshape(shards * CAP, GROUP_EXP)
        start = (group * SPAN).astype(jnp.int32)
        w_gate = lax.dynamic_slice_in_dim(gate_proj, start, SPAN, 0).astype(jnp.float32)
        w_up = lax.dynamic_slice_in_dim(up_proj, start, SPAN, 0).astype(jnp.float32)
        w_down = lax.dynamic_slice_in_dim(down_proj, start, SPAN, 0).astype(jnp.float32)
        gate_h = jnp.einsum('rd,pdc->rpc', rows, w_gate)
        up_h = jnp.einsum('rd,pdc->rpc', rows, w_up)
        hidden = (jax.nn.silu(gate_h) * up_h).reshape(shards * CAP, SPAN, GROUP_EXP, HSLICE)
        hidden = hidden * row_factor[:, None, :, None]
        hidden = lax.optimization_barrier(hidden.astype(jnp.bfloat16)).astype(jnp.float32)
        hidden = hidden.reshape(shards * CAP, SPAN, width_cols)
        result = jnp.einsum('rpc,pdc->rd', hidden, w_down)
        result = lax.optimization_barrier(result.astype(jnp.bfloat16)).astype(jnp.float32)
        result = result.reshape(shards, CAP, D)
        return total + jnp.einsum('stc,scd->std', select, result), None

    start_total = jnp.zeros((shards, TOK_DEV, D), jnp.float32)
    total, unused = lax.scan(one_group, start_total, jnp.arange(GROUPS, dtype=jnp.int32))
    return total.reshape(TOKENS, D).astype(jnp.bfloat16)
```

```python
import functools

import jax
import jax.numpy as jnp
from jax import lax
from jax.experimental import pallas as pl
from jax.experimental.pallas import tpu as pltpu
from jax.sharding import PartitionSpec as P

GROUP_EXP = 3
SPAN = 4
CAP = 8
LANES = 128
CHUNK = 16


def select_rows(group_ids, home, n_groups):
    tok_rows = group_ids.shape[1]
    n_rows = n_groups * CAP
    row = lax.broadcasted_iota(jnp.int32, (n_rows, tok_rows), 0)
    group = lax.rem(home + row // CAP, n_groups)
    member = jnp.zeros((n_rows, tok_rows), jnp.float32)
    for j in range(group_ids.shape[0]):
        member += (group_ids[j : j + 1, :] == group).astype(jnp.float32)
    first = lax.broadcasted_iota(jnp.int32, (tok_rows, tok_rows), 0)
    second = lax.broadcasted_iota(jnp.int32, (tok_rows, tok_rows), 1)
    earlier = (first < second).astype(jnp.bfloat16)
    rank = jnp.dot(member.astype(jnp.bfloat16), earlier, preferred_element_type=jnp.float32)
    slot = (row % CAP).astype(jnp.float32)
    return jnp.where(rank == slot, member, 0.0)


def expert_weights(expert_ids, gate_weights, home, n_groups, lanes):
    tok_rows = expert_ids.shape[1]
    row = lax.broadcasted_iota(jnp.int32, (lanes, tok_rows), 0)
    group = lax.rem(home + row // GROUP_EXP, n_groups)
    expert = jnp.where(row < n_groups * GROUP_EXP, group * GROUP_EXP + row % GROUP_EXP, -1)
    total = jnp.zeros((lanes, tok_rows), jnp.float32)
    for j in range(expert_ids.shape[0]):
        total += jnp.where(expert_ids[j : j + 1, :] == expert, gate_weights[j : j + 1, :], 0.0)
    return total


def kernel(
    n_groups, n_dp,
    gid_ref, eid_ref, gw_ref, tok_hbm, wg_hbm, wu_hbm, wd_hbm, out_ref,
    tok, wg, wu, wd, sbuf, abuf, rows, part, got_part, hid, back, shares, summed, final,
    lsem, own_sem, a_send, a_recv, b_send, b_recv, p_send, p_recv, h_send, h_recv,
    q_send, q_recv, c_send, c_recv,
):
    place = lax.axis_index("expert")
    core = lax.axis_index("dp")
    home = place // SPAN
    spot = place % SPAN
    half = tok.shape[1] // n_dp
    lanes = sbuf.shape[3] - half
    cols = wg.shape[1]
    wide = cols // GROUP_EXP

    loads = [
        pltpu.make_async_copy(src, dst, lsem.at[i])
        for i, (src, dst) in enumerate(
            [(tok_hbm, tok), (wg_hbm.at[0], wg), (wu_hbm.at[0], wu), (wd_hbm.at[0], wd)]
        )
    ]
    for load in loads:
        load.start()

    def member(dm, dd):
        return {"expert": home * SPAN + lax.rem(spot + dm, SPAN), "dp": lax.rem(core + dd, n_dp)}

    def group_peer(r):
        return {"expert": lax.rem(home + r, n_groups) * SPAN + spot, "dp": core}

    others = [(dm, dd) for dd in range(n_dp) for dm in range(SPAN) if (dm, dd) != (0, 0)]
    barrier = pltpu.get_barrier_semaphore()
    for r in range(1, n_groups):
        pl.semaphore_signal(barrier, inc=1, device_id=group_peer(r))
    for dm, dd in others:
        pl.semaphore_signal(barrier, inc=1, device_id=member(dm, dd))

    select = select_rows(gid_ref[...], home, n_groups)
    select_low = select.astype(jnp.bfloat16)
    weights = expert_weights(
        eid_ref[...], gw_ref[...].astype(jnp.float32), home, n_groups, lanes
    ).astype(jnp.bfloat16)
    factor = lax.dot_general(
        select_low, weights, (((1,), (1,)), ((), ())), preferred_element_type=jnp.float32
    )
    factor = factor.reshape(n_groups, CAP, lanes).astype(jnp.bfloat16)
    loads[0].wait()
    for h in range(n_dp):
        picked = jnp.dot(
            select_low, tok[:, h * half : (h + 1) * half], preferred_element_type=jnp.float32
        )
        sbuf[h, :, :, :half] = picked.reshape(n_groups, CAP, half).astype(jnp.bfloat16)
        sbuf[h, :, :, half:] = factor
    pl.semaphore_wait(barrier, n_groups - 1 + len(others))

    def remote(src, dst, send, recv, device):
        return pltpu.make_async_remote_copy(
            src_ref=src, dst_ref=dst, send_sem=send, recv_sem=recv,
            device_id=device, device_id_type=pl.DeviceIdType.MESH,
        )

    to_groups = [
        remote(sbuf.at[:, r], abuf.at[:, r], a_send.at[r], a_recv.at[r], group_peer(r))
        for r in range(1, n_groups)
    ]
    for copy in to_groups:
        copy.start()
    near = pl.ds(0, 1)
    far = pl.ds(1, n_groups - 1)

    def spread(src, part_rows, n):
        return [
            remote(
                src.at[lax.rem(core + dd, n_dp), part_rows], rows.at[dd, dm, part_rows],
                b_send.at[n, dd * SPAN + dm], b_recv.at[n, dd * SPAN + dm], member(dm, dd),
            )
            for dm, dd in others
        ]

    near_copies = spread(sbuf, near, 0)
    for copy in near_copies:
        copy.start()
    own_near = pltpu.make_async_copy(sbuf.at[core, near], rows.at[0, 0, near], own_sem.at[0])
    own_near.start()
    far_copies = []
    if n_groups > 1:
        for copy in to_groups:
            copy.wait_recv()
        far_copies = spread(abuf, far, 1)
        for copy in far_copies:
            copy.start()
        own_far = pltpu.make_async_copy(abuf.at[core, far], rows.at[0, 0, far], own_sem.at[1])
        own_far.start()
    loads[1].wait()
    loads[2].wait()
    loads[3].wait()
    own_near.wait()
    if n_groups > 1:
        own_far.wait()
    for copy in near_copies + far_copies:
        copy.wait_recv()

    n_units = n_dp * SPAN * n_groups
    n_rows = n_units * CAP
    half_rows = n_rows // n_dp
    units = rows.reshape(n_units, CAP, half + lanes)

    def chunked(total, step, work):
        if total <= step:
            work(0, total)
        else:

            @pl.loop(0, total // step)
            def _(i):
                work(i * step, step)

    other_core = member(0, 1)
    exchange = []
    for which, w in ((0, wg), (1, wu)):

        def project(start, size, which=which, w=w):
            block = units[pl.ds(start, size), :, :half].astype(jnp.float32)
            block = block.reshape(size * CAP, half).astype(jnp.bfloat16)
            part[which, pl.ds(pl.multiple_of(start * CAP, CAP), size * CAP), :] = jnp.dot(
                block, w[...], preferred_element_type=jnp.float32
            )

        chunked(n_units, CHUNK, project)
        copy = remote(
            part.at[which, pl.ds(half_rows, half_rows)], got_part.at[which],
            p_send.at[which], p_recv.at[which], other_core,
        )
        copy.start()
        exchange.append(copy)
    for copy in exchange:
        copy.wait_recv()

    def activate(start, size):
        count = size * CAP
        at = pl.ds(pl.multiple_of(start * CAP, CAP), count)
        gate_h = part[0, at, :] + got_part[0, at, :]
        up_h = part[1, at, :] + got_part[1, at, :]
        weight = units[pl.ds(start, size), :, half:].astype(jnp.float32).reshape(count, lanes)
        row = lax.broadcasted_iota(jnp.int32, (count, lanes), 0) + start * CAP
        lane = lax.broadcasted_iota(jnp.int32, (count, lanes), 1)
        first = row // CAP % n_groups * GROUP_EXP
        col = lax.broadcasted_iota(jnp.int32, (count, cols), 1)
        scale = jnp.zeros((count, cols), jnp.float32)
        for k in range(GROUP_EXP):
            one = jnp.sum(jnp.where(lane == first + k, weight, 0.0), axis=1, keepdims=True)
            scale = jnp.where(col // wide == k, one, scale)
        active = gate_h / (1.0 + jnp.exp(-gate_h)) * up_h
        hid[0, at, :] = (active * scale).astype(jnp.bfloat16)

    chunked(n_units // n_dp, CHUNK, activate)
    hidden_copy = remote(hid.at[0], hid.at[1], h_send, h_recv, other_core)
    hidden_copy.start()
    shares_units = back.reshape(n_units, CAP, half)

    def lower(which):
        def work(start, size):
            at = pl.ds(pl.multiple_of(start * CAP, CAP), size * CAP)
            value = lax.dot_general(
                hid[which, at, :], wd[...], (((1,), (1,)), ((), ())),
                preferred_element_type=jnp.float32,
            )
            shares_units[pl.ds(start + which * (n_units // n_dp), size)] = value.reshape(
                size, CAP, half
            ).astype(jnp.bfloat16)

        chunked(n_units // n_dp, CHUNK, work)

    returns = {}
    for dd in range(n_dp):
        if dd == 1:
            hidden_copy.wait_recv()
        lower(dd)
        for n, part_rows in ((1, far), (0, near)):
            if n == 1 and n_groups == 1:
                continue
            for dm in range(SPAN):
                if (dm, dd) == (0, 0):
                    continue
                returns[n, dm, dd] = remote(
                    back.at[dd, dm, part_rows], shares.at[dd, dm, part_rows],
                    q_send.at[n, dd * SPAN + dm], q_recv.at[n, dd * SPAN + dm],
                    member(SPAN - dm, n_dp - dd),
                )
                returns[n, dm, dd].start()

    def reduce(dd, part_rows):
        total = None
        for dm in range(SPAN):
            src = back if (dm, dd) == (0, 0) else shares
            value = src[dd, dm, part_rows].astype(jnp.float32)
            total = value if total is None else total + value
        return total.astype(jnp.bfloat16)

    homeward = []
    if n_groups > 1:
        for dm, dd in others:
            returns[1, dm, dd].wait_recv()
        for dd in range(n_dp):
            summed[dd, far] = reduce(dd, far)
        homeward = [
            remote(
                summed.at[:, r], final.at[:, r], c_send.at[r], c_recv.at[r],
                group_peer(n_groups - r),
            )
            for r in range(1, n_groups)
        ]
        for copy in homeward:
            copy.start()
    for dm, dd in others:
        returns[0, dm, dd].wait_recv()
    for dd in range(n_dp):
        final[dd, near] = reduce(dd, near)
    for copy in homeward:
        copy.wait_recv()
    for dd in range(n_dp):
        block = final[dd].astype(jnp.float32).reshape(n_groups * CAP, half).astype(jnp.bfloat16)
        value = lax.dot_general(
            select_low, block, (((0,), (0,)), ((), ())), preferred_element_type=jnp.float32
        )
        at = pl.multiple_of(lax.rem(core + dd, n_dp) * half, LANES)
        out_ref[:, pl.ds(at, half)] = value.astype(jnp.bfloat16)
    for copy in to_groups + near_copies + far_copies + exchange + [hidden_copy]:
        copy.wait_send()
    for copy in list(returns.values()) + homeward:
        copy.wait_send()


def body(tokens, group_ids, expert_ids, gate_weights, gate_proj, up_proj, down_proj):
    tok_rows, width = tokens.shape
    n_groups = lax.axis_size("expert") // SPAN
    n_dp = lax.axis_size("dp")
    half = gate_proj.shape[1]
    cols = gate_proj.shape[2]
    lanes = -(-n_groups * GROUP_EXP // LANES) * LANES
    n_rows = n_dp * SPAN * n_groups * CAP
    low, full = jnp.bfloat16, jnp.float32
    vmem = pl.BlockSpec(memory_space=pltpu.VMEM)
    hbm = pl.BlockSpec(memory_space=pl.ANY)
    dma = pltpu.SemaphoreType.DMA
    spots = n_dp * SPAN
    return pl.pallas_call(
        functools.partial(kernel, n_groups, n_dp),
        out_shape=jax.ShapeDtypeStruct((tok_rows, width), low),
        in_specs=[vmem, vmem, vmem, hbm, hbm, hbm, hbm],
        out_specs=vmem,
        scratch_shapes=[
            pltpu.VMEM((tok_rows, width), low),
            pltpu.VMEM((half, cols), low),
            pltpu.VMEM((half, cols), low),
            pltpu.VMEM((half, cols), low),
            pltpu.VMEM((n_dp, n_groups, CAP, half + lanes), low),
            pltpu.VMEM((n_dp, n_groups, CAP, half + lanes), low),
            pltpu.VMEM((n_dp, SPAN, n_groups, CAP, half + lanes), low),
            pltpu.VMEM((2, n_rows, cols), full),
            pltpu.VMEM((2, n_rows // n_dp, cols), full),
            pltpu.VMEM((n_dp, n_rows // n_dp, cols), low),
            pltpu.VMEM((n_dp, SPAN, n_groups, CAP, half), low),
            pltpu.VMEM((n_dp, SPAN, n_groups, CAP, half), low),
            pltpu.VMEM((n_dp, n_groups, CAP, half), low),
            pltpu.VMEM((n_dp, n_groups, CAP, half), low),
            dma((4,)), dma((2,)),
            dma((n_groups,)), dma((n_groups,)),
            dma((2, spots)), dma((2, spots)),
            dma((2,)), dma((2,)), dma, dma,
            dma((2, spots)), dma((2, spots)),
            dma((n_groups,)), dma((n_groups,)),
        ],
        compiler_params=pltpu.CompilerParams(
            collective_id=0, has_side_effects=True, vmem_limit_bytes=60 * 1024 * 1024
        ),
    )(group_ids.T, expert_ids.T, gate_weights.T, tokens, gate_proj, up_proj, down_proj)


def solution(mesh):
    placed = (
        P(("groups", "expert", "dp"), None),
        P(("groups", "expert", "dp"), None),
        P(("groups", "expert", "dp"), None),
        P(("groups", "expert", "dp"), None),
        P("expert", "dp", None),
        P("expert", "dp", None),
        P("expert", "dp", None),
    )
    return jax.shard_map(
        body,
        mesh=mesh,
        in_specs=placed,
        out_specs=P(("groups", "expert", "dp"), None),
        check_vma=False,
    )
```

```python
import functools

import jax
import jax.numpy as jnp
from jax import lax
from jax.experimental import pallas as pl
from jax.experimental.pallas import tpu as pltpu
from jax.sharding import PartitionSpec as P

GROUP_EXP = 3
SPAN = 4
CAP = 8
LANES = 128


def select_rows(group_ids, home, n_groups):
    tok_rows = group_ids.shape[1]
    n_rows = n_groups * CAP
    row = lax.broadcasted_iota(jnp.int32, (n_rows, tok_rows), 0)
    group = lax.rem(home + row // CAP, n_groups)
    member = jnp.zeros((n_rows, tok_rows), jnp.float32)
    for j in range(group_ids.shape[0]):
        member += (group_ids[j : j + 1, :] == group).astype(jnp.float32)
    first = lax.broadcasted_iota(jnp.int32, (tok_rows, tok_rows), 0)
    second = lax.broadcasted_iota(jnp.int32, (tok_rows, tok_rows), 1)
    earlier = (first < second).astype(jnp.bfloat16)
    rank = jnp.dot(member.astype(jnp.bfloat16), earlier, preferred_element_type=jnp.float32)
    slot = (row % CAP).astype(jnp.float32)
    return jnp.where(rank == slot, member, 0.0)


def expert_weights(expert_ids, gate_weights, home, n_groups, lanes):
    tok_rows = expert_ids.shape[1]
    row = lax.broadcasted_iota(jnp.int32, (lanes, tok_rows), 0)
    group = lax.rem(home + row // GROUP_EXP, n_groups)
    expert = jnp.where(row < n_groups * GROUP_EXP, group * GROUP_EXP + row % GROUP_EXP, -1)
    total = jnp.zeros((lanes, tok_rows), jnp.float32)
    for j in range(expert_ids.shape[0]):
        total += jnp.where(expert_ids[j : j + 1, :] == expert, gate_weights[j : j + 1, :], 0.0)
    return total


def kernel(
    n_groups, n_dp,
    gid_ref, eid_ref, gw_ref, tok_hbm, wg_hbm, wu_hbm, wd_hbm, out_ref,
    tok, wg, wu, wd, sbuf, abuf, summed, final, near_bufs, far_bufs,
    lsem, own_sem, a_send, a_recv, b_send, b_recv, p_send, p_recv, h_send, h_recv,
    q_send, q_recv, c_send, c_recv,
):
    place = lax.axis_index("expert")
    core = lax.axis_index("dp")
    home = place // SPAN
    spot = place % SPAN
    half = tok.shape[1] // n_dp
    lanes = sbuf.shape[3] - half
    cols = wg.shape[0]
    wide = cols // GROUP_EXP

    loads = [
        pltpu.make_async_copy(src, dst, lsem.at[i])
        for i, (src, dst) in enumerate(
            [(tok_hbm, tok), (wg_hbm.at[0], wg), (wu_hbm.at[0], wu), (wd_hbm.at[0], wd)]
        )
    ]
    for load in loads:
        load.start()

    def member(dm, dd):
        return {"expert": home * SPAN + lax.rem(spot + dm, SPAN), "dp": lax.rem(core + dd, n_dp)}

    def group_peer(r):
        return {"expert": lax.rem(home + r, n_groups) * SPAN + spot, "dp": core}

    others = [(dm, dd) for dd in range(n_dp) for dm in range(SPAN) if (dm, dd) != (0, 0)]
    barrier = pltpu.get_barrier_semaphore()
    for r in range(1, n_groups):
        pl.semaphore_signal(barrier, inc=1, device_id=group_peer(r))
    for dm, dd in others:
        pl.semaphore_signal(barrier, inc=1, device_id=member(dm, dd))

    select = select_rows(gid_ref[...], home, n_groups)
    select_low = select.astype(jnp.bfloat16)
    weights = expert_weights(
        eid_ref[...], gw_ref[...].astype(jnp.float32), home, n_groups, lanes
    ).astype(jnp.bfloat16)
    factor = lax.dot_general(
        select_low, weights, (((1,), (1,)), ((), ())), preferred_element_type=jnp.float32
    )
    factor = factor.reshape(n_groups, CAP, lanes).astype(jnp.bfloat16)
    loads[0].wait()
    for h in range(n_dp):
        picked = jnp.dot(
            select_low, tok[:, h * half : (h + 1) * half], preferred_element_type=jnp.float32
        )
        sbuf[h, :, :, :half] = picked.reshape(n_groups, CAP, half).astype(jnp.bfloat16)
        sbuf[h, :, :, half:] = factor
    pl.semaphore_wait(barrier, n_groups - 1 + len(others))

    def remote(src, dst, send, recv, device):
        return pltpu.make_async_remote_copy(
            src_ref=src, dst_ref=dst, send_sem=send, recv_sem=recv,
            device_id=device, device_id_type=pl.DeviceIdType.MESH,
        )

    others.sort(key=lambda pair: pair[1])
    n_far = n_groups - 1

    def turn(dd):
        return lax.rem(core + dd, n_dp)

    to_groups = {}
    for dd in range(n_dp):
        for r in range(1, n_groups):
            to_groups[dd, r] = remote(
                sbuf.at[turn(dd), r], abuf.at[turn(dd), r - 1],
                a_send.at[dd, r - 1], a_recv.at[dd, r - 1], group_peer(r),
            )
            to_groups[dd, r].start()

    other_core = member(0, 1)
    started = list(to_groups.values())

    def begin(*args):
        copy = remote(*args)
        copy.start()
        started.append(copy)
        return copy

    def chunked(total, step, work):
        if total <= step:
            work(0, total)
        else:

            @pl.loop(0, total // step)
            def _(i):
                work(i * step, step)

    def spread(n, dd, rows):
        src = sbuf.at[turn(dd), pl.ds(0, 1)] if n == 0 else abuf.at[turn(dd)]
        copies = []
        if dd == 0:
            own = pltpu.make_async_copy(src, rows.at[0, 0], own_sem.at[n])
            own.start()
            copies.append(own)
        for dm in range(SPAN):
            if (dm, dd) != (0, 0):
                spot_at = dd * SPAN + dm
                copies.append(
                    begin(
                        src, rows.at[dd, dm], b_send.at[n, spot_at], b_recv.at[n, spot_at],
                        member(dm, dd),
                    )
                )
        return copies

    def settle(copies):
        for copy in copies:
            if copy.is_remote:
                copy.wait_recv()
            else:
                copy.wait()

    def work_on(n, first_group, count, bufs):
        rows, part, got_part, hid, back, shares = bufs
        n_units = n_dp * SPAN * count
        half_units = n_units // n_dp
        half_rows = half_units * CAP
        units = rows.reshape(n_units, CAP, half + lanes)
        back_units = back.reshape(n_units, CAP, half)
        exchange = []
        for which, w in ((0, wg), (1, wu)):

            def project(start, size, which=which, w=w):
                block = units[pl.ds(start, size), :, :half].astype(jnp.float32)
                block = block.reshape(size * CAP, half).astype(jnp.bfloat16)
                part[which, pl.ds(pl.multiple_of(start * CAP, CAP), size * CAP), :] = (
                    lax.dot_general(
                        block, w[...], (((1,), (1,)), ((), ())),
                        preferred_element_type=jnp.float32,
                    )
                )

            chunked(n_units, n_dp * SPAN, project)
            exchange.append(
                begin(
                    part.at[which, pl.ds(half_rows, half_rows)], got_part.at[which],
                    p_send.at[n, which], p_recv.at[n, which], other_core,
                )
            )
        settle(exchange)

        def activate(start, size):
            total = size * CAP
            at = pl.ds(pl.multiple_of(start * CAP, CAP), total)
            gate_h = part[0, at, :] + got_part[0, at, :]
            up_h = part[1, at, :] + got_part[1, at, :]
            weight = units[pl.ds(start, size), :, half:].astype(jnp.float32)
            weight = weight.reshape(total, lanes)
            row = lax.broadcasted_iota(jnp.int32, (total, lanes), 0) + start * CAP
            lane = lax.broadcasted_iota(jnp.int32, (total, lanes), 1)
            first = (first_group + row // CAP % count) * GROUP_EXP
            col = lax.broadcasted_iota(jnp.int32, (total, cols), 1)
            scale = jnp.zeros((total, cols), jnp.float32)
            for k in range(GROUP_EXP):
                one = jnp.sum(jnp.where(lane == first + k, weight, 0.0), axis=1, keepdims=True)
                scale = jnp.where(col // wide == k, one, scale)
            active = gate_h / (1.0 + jnp.exp(-gate_h)) * up_h
            hid[0, at, :] = (active * scale).astype(jnp.bfloat16)

        chunked(half_units, SPAN, activate)
        hidden_copy = begin(hid.at[0], hid.at[1], h_send.at[n], h_recv.at[n], other_core)

        def lower(which):
            def work(start, size):
                at = pl.ds(pl.multiple_of(start * CAP, CAP), size * CAP)
                value = jnp.dot(hid[which, at, :], wd[...], preferred_element_type=jnp.float32)
                back_units[pl.ds(start + which * half_units, size)] = value.reshape(
                    size, CAP, half
                ).astype(jnp.bfloat16)

            chunked(half_units, SPAN, work)

        returns = {}
        for dd in range(n_dp):
            if dd == 1:
                settle([hidden_copy])
            lower(dd)
            for dm in range(SPAN):
                if (dm, dd) != (0, 0):
                    spot_at = dd * SPAN + dm
                    returns[dm, dd] = begin(
                        back.at[dd, dm], shares.at[dd, dm],
                        q_send.at[n, spot_at], q_recv.at[n, spot_at],
                        member(SPAN - dm, n_dp - dd),
                    )
        return returns

    def reduce(dd, bufs, returns):
        settle([returns[dm, dd] for dm in range(SPAN) if (dm, dd) in returns])
        total = None
        for dm in range(SPAN):
            src = bufs[4] if (dm, dd) == (0, 0) else bufs[5]
            value = src[dd, dm].astype(jnp.float32)
            total = value if total is None else total + value
        return total.astype(jnp.bfloat16)

    near_copies = spread(0, 0, near_bufs[0]) + spread(0, 1, near_bufs[0])
    far_copies = []
    for dd in range(n_dp):
        settle([to_groups[dd, r] for r in range(1, n_groups)])
        far_copies += spread(1, dd, far_bufs[0])
    for load in loads[1:]:
        load.wait()
    settle(near_copies)
    near_returns = work_on(0, 0, 1, near_bufs)
    settle(far_copies)
    far_returns = work_on(1, 1, n_far, far_bufs)
    for dd in range(n_dp):
        final[dd, pl.ds(0, 1)] = reduce(dd, near_bufs, near_returns)
    homeward = []
    for dd in range(n_dp):
        summed[dd] = reduce(dd, far_bufs, far_returns)
        for r in range(1, n_groups):
            homeward.append(
                begin(
                    summed.at[dd, r - 1], final.at[dd, r], c_send.at[dd, r - 1],
                    c_recv.at[dd, r - 1], group_peer(n_groups - r),
                )
            )
    for dd in range(n_dp):
        settle(homeward[dd * n_far : (dd + 1) * n_far])
        block = final[dd].astype(jnp.float32).reshape(n_groups * CAP, half).astype(jnp.bfloat16)
        value = lax.dot_general(
            select_low, block, (((0,), (0,)), ((), ())), preferred_element_type=jnp.float32
        )
        at = pl.multiple_of(turn(dd) * half, LANES)
        out_ref[:, pl.ds(at, half)] = value.astype(jnp.bfloat16)
    for copy in started:
        copy.wait_send()


def body(tokens, group_ids, expert_ids, gate_weights, gate_proj, up_proj, down_proj):
    tok_rows, width = tokens.shape
    n_groups = lax.axis_size("expert") // SPAN
    n_dp = lax.axis_size("dp")
    half = gate_proj.shape[1]
    cols = gate_proj.shape[2]
    lanes = -(-n_groups * GROUP_EXP // LANES) * LANES
    low, full = jnp.bfloat16, jnp.float32
    vmem = pl.BlockSpec(memory_space=pltpu.VMEM)
    hbm = pl.BlockSpec(memory_space=pl.ANY)
    dma = pltpu.SemaphoreType.DMA
    spots = n_dp * SPAN

    def buffers(count):
        n_rows = n_dp * SPAN * count * CAP
        return (
            pltpu.VMEM((n_dp, SPAN, count, CAP, half + lanes), low),
            pltpu.VMEM((2, n_rows, cols), full),
            pltpu.VMEM((2, n_rows // n_dp, cols), full),
            pltpu.VMEM((n_dp, n_rows // n_dp, cols), low),
            pltpu.VMEM((n_dp, SPAN, count, CAP, half), low),
            pltpu.VMEM((n_dp, SPAN, count, CAP, half), low),
        )

    return pl.pallas_call(
        functools.partial(kernel, n_groups, n_dp),
        out_shape=jax.ShapeDtypeStruct((tok_rows, width), low),
        in_specs=[vmem, vmem, vmem, hbm, hbm, hbm, hbm],
        out_specs=vmem,
        scratch_shapes=[
            pltpu.VMEM((tok_rows, width), low),
            pltpu.VMEM((cols, half), low),
            pltpu.VMEM((cols, half), low),
            pltpu.VMEM((cols, half), low),
            pltpu.VMEM((n_dp, n_groups, CAP, half + lanes), low),
            pltpu.VMEM((n_dp, n_groups - 1, CAP, half + lanes), low),
            pltpu.VMEM((n_dp, n_groups - 1, CAP, half), low),
            pltpu.VMEM((n_dp, n_groups, CAP, half), low),
            buffers(1),
            buffers(n_groups - 1),
            dma((4,)), dma((2,)),
            dma((n_dp, n_groups - 1)), dma((n_dp, n_groups - 1)),
            dma((2, spots)), dma((2, spots)),
            dma((2, 2)), dma((2, 2)), dma((2,)), dma((2,)),
            dma((2, spots)), dma((2, spots)),
            dma((n_dp, n_groups - 1)), dma((n_dp, n_groups - 1)),
        ],
        compiler_params=pltpu.CompilerParams(
            collective_id=0, has_side_effects=True, vmem_limit_bytes=60 * 1024 * 1024
        ),
    )(group_ids.T, expert_ids.T, gate_weights.T, tokens,
      *(jnp.swapaxes(w, 1, 2) for w in (gate_proj, up_proj, down_proj)))


def solution(mesh):
    placed = (
        P(("groups", "expert", "dp"), None),
        P(("groups", "expert", "dp"), None),
        P(("groups", "expert", "dp"), None),
        P(("groups", "expert", "dp"), None),
        P("expert", "dp", None),
        P("expert", "dp", None),
        P("expert", "dp", None),
    )
    return jax.shard_map(
        body,
        mesh=mesh,
        in_specs=placed,
        out_specs=P(("groups", "expert", "dp"), None),
        check_vma=False,
    )
```

```python
import functools

import jax
import jax.numpy as jnp
from jax import lax
from jax.experimental import pallas as pl
from jax.experimental.pallas import tpu as pltpu
from jax.sharding import PartitionSpec as P

GROUP_EXP = 3
SPAN = 4
CAP = 8
LANES = 128


def select_rows(group_ids, home, n_groups):
    tok_rows = group_ids.shape[1]
    n_rows = n_groups * CAP
    row = lax.broadcasted_iota(jnp.int32, (n_rows, tok_rows), 0)
    group = lax.rem(home + row // CAP, n_groups)
    member = jnp.zeros((n_rows, tok_rows), jnp.float32)
    for j in range(group_ids.shape[0]):
        member += (group_ids[j : j + 1, :] == group).astype(jnp.float32)
    first = lax.broadcasted_iota(jnp.int32, (tok_rows, tok_rows), 0)
    second = lax.broadcasted_iota(jnp.int32, (tok_rows, tok_rows), 1)
    earlier = (first < second).astype(jnp.bfloat16)
    rank = jnp.dot(member.astype(jnp.bfloat16), earlier, preferred_element_type=jnp.float32)
    slot = (row % CAP).astype(jnp.float32)
    return jnp.where(rank == slot, member, 0.0)


def expert_weights(expert_ids, gate_weights, home, n_groups, lanes):
    tok_rows = expert_ids.shape[1]
    row = lax.broadcasted_iota(jnp.int32, (lanes, tok_rows), 0)
    group = lax.rem(home + row // GROUP_EXP, n_groups)
    expert = jnp.where(row < n_groups * GROUP_EXP, group * GROUP_EXP + row % GROUP_EXP, -1)
    total = jnp.zeros((lanes, tok_rows), jnp.float32)
    for j in range(expert_ids.shape[0]):
        total += jnp.where(expert_ids[j : j + 1, :] == expert, gate_weights[j : j + 1, :], 0.0)
    return total


def kernel(
    n_groups, n_dp,
    gid_ref, eid_ref, gw_ref, tok_hbm, wg_hbm, wu_hbm, wd_hbm, out_ref, select_ref,
    tok, wg, wu, wd, sbuf, abuf, summed, final, near_bufs, far_bufs,
    lsem, own_sem, a_send, a_recv, b_send, b_recv, p_send, p_recv, h_send, h_recv,
    q_send, q_recv, c_send, c_recv,
):
    place = lax.axis_index("expert")
    core = lax.axis_index("dp")
    home = place // SPAN
    spot = place % SPAN
    half = tok.shape[1] // n_dp
    lanes = sbuf.shape[3] - half
    cols = wg.shape[0]
    wide = cols // GROUP_EXP

    loads = [
        pltpu.make_async_copy(src, dst, lsem.at[i])
        for i, (src, dst) in enumerate(
            [(tok_hbm, tok), (wg_hbm.at[0], wg), (wu_hbm.at[0], wu), (wd_hbm.at[0], wd)]
        )
    ]
    for load in loads:
        load.start()

    def member(dm, dd):
        return {"expert": home * SPAN + lax.rem(spot + dm, SPAN), "dp": lax.rem(core + dd, n_dp)}

    def group_peer(r):
        return {"expert": lax.rem(home + r, n_groups) * SPAN + spot, "dp": core}

    others = [(dm, dd) for dd in range(n_dp) for dm in range(SPAN) if (dm, dd) != (0, 0)]
    barrier = pltpu.get_barrier_semaphore()
    for r in range(1, n_groups):
        pl.semaphore_signal(barrier, inc=1, device_id=group_peer(r))
    for dm, dd in others:
        pl.semaphore_signal(barrier, inc=1, device_id=member(dm, dd))

    select = select_rows(gid_ref[...], home, n_groups)
    select_low = select.astype(jnp.bfloat16)
    select_ref[...] = select_low
    weights = expert_weights(
        eid_ref[...], gw_ref[...].astype(jnp.float32), home, n_groups, lanes
    ).astype(jnp.bfloat16)
    factor = lax.dot_general(
        select_low, weights, (((1,), (1,)), ((), ())), preferred_element_type=jnp.float32
    )
    factor = factor.reshape(n_groups, CAP, lanes).astype(jnp.bfloat16)
    loads[0].wait()
    for h in range(n_dp):
        picked = jnp.dot(
            select_low, tok[:, h * half : (h + 1) * half], preferred_element_type=jnp.float32
        )
        sbuf[h, :, :, :half] = picked.reshape(n_groups, CAP, half).astype(jnp.bfloat16)
        sbuf[h, :, :, half:] = factor
    pl.semaphore_wait(barrier, n_groups - 1 + len(others))

    def remote(src, dst, send, recv, device):
        return pltpu.make_async_remote_copy(
            src_ref=src, dst_ref=dst, send_sem=send, recv_sem=recv,
            device_id=device, device_id_type=pl.DeviceIdType.MESH,
        )

    others.sort(key=lambda pair: pair[1])
    n_far = n_groups - 1

    def turn(dd):
        return lax.rem(core + dd, n_dp)

    to_groups = {}
    for dd in range(n_dp):
        for r in range(1, n_groups):
            to_groups[dd, r] = remote(
                sbuf.at[turn(dd), r], abuf.at[turn(dd), r - 1],
                a_send.at[dd, r - 1], a_recv.at[dd, r - 1], group_peer(r),
            )
            to_groups[dd, r].start()

    other_core = member(0, 1)
    started = list(to_groups.values())

    def begin(*args):
        copy = remote(*args)
        copy.start()
        started.append(copy)
        return copy

    def chunked(total, step, work):
        if total <= step:
            work(0, total)
        else:

            @pl.loop(0, total // step)
            def _(i):
                work(i * step, step)

    def spread(n, dd, rows):
        src = sbuf.at[turn(dd), pl.ds(0, 1)] if n == 0 else abuf.at[turn(dd)]
        copies = []
        if dd == 0:
            own = pltpu.make_async_copy(src, rows.at[0, 0], own_sem.at[n])
            own.start()
            copies.append(own)
        for dm in range(SPAN):
            if (dm, dd) != (0, 0):
                spot_at = dd * SPAN + dm
                copies.append(
                    begin(
                        src, rows.at[dd, dm], b_send.at[n, spot_at], b_recv.at[n, spot_at],
                        member(dm, dd),
                    )
                )
        return copies

    def settle(copies):
        for copy in copies:
            if copy.is_remote:
                copy.wait_recv()
            else:
                copy.wait()

    def work_on(n, first_group, count, bufs):
        rows, part, got_part, hid, back, shares = bufs
        n_units = n_dp * SPAN * count
        half_units = n_units // n_dp
        half_rows = half_units * CAP
        units = rows.reshape(n_units, CAP, half + lanes)
        back_units = back.reshape(n_units, CAP, half)
        exchange = []
        for which, w in ((0, wg), (1, wu)):

            def project(start, size, which=which, w=w):
                block = units[pl.ds(start, size), :, :half].astype(jnp.float32)
                block = block.reshape(size * CAP, half).astype(jnp.bfloat16)
                part[which, pl.ds(pl.multiple_of(start * CAP, CAP), size * CAP), :] = (
                    lax.dot_general(
                        block, w[...], (((1,), (1,)), ((), ())),
                        preferred_element_type=jnp.float32,
                    )
                )

            chunked(n_units, n_dp * SPAN, project)
            exchange.append(
                begin(
                    part.at[which, pl.ds(half_rows, half_rows)], got_part.at[which],
                    p_send.at[n, which], p_recv.at[n, which], other_core,
                )
            )
        settle(exchange)

        def activate(start, size):
            total = size * CAP
            at = pl.ds(pl.multiple_of(start * CAP, CAP), total)
            gate_h = part[0, at, :] + got_part[0, at, :]
            up_h = part[1, at, :] + got_part[1, at, :]
            weight = units[pl.ds(start, size), :, half:].astype(jnp.float32)
            weight = weight.reshape(total, lanes)
            row = lax.broadcasted_iota(jnp.int32, (total, lanes), 0) + start * CAP
            lane = lax.broadcasted_iota(jnp.int32, (total, lanes), 1)
            first = (first_group + row // CAP % count) * GROUP_EXP
            col = lax.broadcasted_iota(jnp.int32, (total, cols), 1)
            scale = jnp.zeros((total, cols), jnp.float32)
            for k in range(GROUP_EXP):
                one = jnp.sum(jnp.where(lane == first + k, weight, 0.0), axis=1, keepdims=True)
                scale = jnp.where(col // wide == k, one, scale)
            active = gate_h / (1.0 + jnp.exp(-gate_h)) * up_h
            hid[0, at, :] = (active * scale).astype(jnp.bfloat16)

        chunked(half_units, SPAN, activate)
        hidden_copy = begin(hid.at[0], hid.at[1], h_send.at[n], h_recv.at[n], other_core)

        def lower(which):
            def work(start, size):
                at = pl.ds(pl.multiple_of(start * CAP, CAP), size * CAP)
                value = jnp.dot(hid[which, at, :], wd[...], preferred_element_type=jnp.float32)
                back_units[pl.ds(start + which * half_units, size)] = value.reshape(
                    size, CAP, half
                ).astype(jnp.bfloat16)

            chunked(half_units, SPAN, work)

        returns = {}
        for dd in range(n_dp):
            if dd == 1:
                settle([hidden_copy])
            lower(dd)
            for dm in range(SPAN):
                if (dm, dd) != (0, 0):
                    spot_at = dd * SPAN + dm
                    returns[dm, dd] = begin(
                        back.at[dd, dm], shares.at[dd, dm],
                        q_send.at[n, spot_at], q_recv.at[n, spot_at],
                        member(SPAN - dm, n_dp - dd),
                    )
        return returns

    def reduce(dd, bufs, returns):
        settle([returns[dm, dd] for dm in range(SPAN) if (dm, dd) in returns])
        total = None
        for dm in range(SPAN):
            src = bufs[4] if (dm, dd) == (0, 0) else bufs[5]
            value = src[dd, dm].astype(jnp.float32)
            total = value if total is None else total + value
        return total.astype(jnp.bfloat16)

    near_copies = spread(0, 0, near_bufs[0]) + spread(0, 1, near_bufs[0])
    far_copies = []
    for dd in range(n_dp):
        settle([to_groups[dd, r] for r in range(1, n_groups)])
        far_copies += spread(1, dd, far_bufs[0])
    for load in loads[1:]:
        load.wait()
    settle(near_copies)
    near_returns = work_on(0, 0, 1, near_bufs)
    settle(far_copies)
    far_returns = work_on(1, 1, n_far, far_bufs)
    for dd in range(n_dp):
        final[dd, pl.ds(0, 1)] = reduce(dd, near_bufs, near_returns)
    homeward = []
    for dd in range(n_dp):
        summed[dd] = reduce(dd, far_bufs, far_returns)
        for r in range(1, n_groups):
            homeward.append(
                begin(
                    summed.at[dd, r - 1], final.at[dd, r], c_send.at[dd, r - 1],
                    c_recv.at[dd, r - 1], group_peer(n_groups - r),
                )
            )
    for dd in range(n_dp):
        settle(homeward[dd * n_far : (dd + 1) * n_far])
        out_ref[dd] = final[dd]
    for copy in started:
        copy.wait_send()


def combine(n_dp, parts_ref, select_ref, out_ref):
    core = lax.axis_index("dp")
    half = parts_ref.shape[3]
    for dd in range(n_dp):
        block = parts_ref[dd].astype(jnp.float32).reshape(-1, half).astype(jnp.bfloat16)
        value = lax.dot_general(
            select_ref[...], block, (((0,), (0,)), ((), ())), preferred_element_type=jnp.float32
        )
        at = pl.multiple_of(lax.rem(core + dd, n_dp) * half, LANES)
        out_ref[:, pl.ds(at, half)] = value.astype(jnp.bfloat16)


def body(tokens, group_ids, expert_ids, gate_weights, gate_proj, up_proj, down_proj):
    tok_rows, width = tokens.shape
    n_groups = lax.axis_size("expert") // SPAN
    n_dp = lax.axis_size("dp")
    half = gate_proj.shape[1]
    cols = gate_proj.shape[2]
    lanes = -(-n_groups * GROUP_EXP // LANES) * LANES
    low, full = jnp.bfloat16, jnp.float32
    vmem = pl.BlockSpec(memory_space=pltpu.VMEM)
    hbm = pl.BlockSpec(memory_space=pl.ANY)
    dma = pltpu.SemaphoreType.DMA
    spots = n_dp * SPAN

    def buffers(count):
        n_rows = n_dp * SPAN * count * CAP
        return (
            pltpu.VMEM((n_dp, SPAN, count, CAP, half + lanes), low),
            pltpu.VMEM((2, n_rows, cols), full),
            pltpu.VMEM((2, n_rows // n_dp, cols), full),
            pltpu.VMEM((n_dp, n_rows // n_dp, cols), low),
            pltpu.VMEM((n_dp, SPAN, count, CAP, half), low),
            pltpu.VMEM((n_dp, SPAN, count, CAP, half), low),
        )

    parts, select = pl.pallas_call(
        functools.partial(kernel, n_groups, n_dp),
        out_shape=(
            jax.ShapeDtypeStruct((n_dp, n_groups, CAP, half), low),
            jax.ShapeDtypeStruct((n_groups * CAP, tok_rows), low),
        ),
        in_specs=[vmem, vmem, vmem, hbm, hbm, hbm, hbm],
        out_specs=(vmem, vmem),
        scratch_shapes=[
            pltpu.VMEM((tok_rows, width), low),
            pltpu.VMEM((cols, half), low),
            pltpu.VMEM((cols, half), low),
            pltpu.VMEM((cols, half), low),
            pltpu.VMEM((n_dp, n_groups, CAP, half + lanes), low),
            pltpu.VMEM((n_dp, n_groups - 1, CAP, half + lanes), low),
            pltpu.VMEM((n_dp, n_groups - 1, CAP, half), low),
            pltpu.VMEM((n_dp, n_groups, CAP, half), low),
            buffers(1),
            buffers(n_groups - 1),
            dma((4,)), dma((2,)),
            dma((n_dp, n_groups - 1)), dma((n_dp, n_groups - 1)),
            dma((2, spots)), dma((2, spots)),
            dma((2, 2)), dma((2, 2)), dma((2,)), dma((2,)),
            dma((2, spots)), dma((2, spots)),
            dma((n_dp, n_groups - 1)), dma((n_dp, n_groups - 1)),
        ],
        compiler_params=pltpu.CompilerParams(
            collective_id=0, has_side_effects=True, vmem_limit_bytes=60 * 1024 * 1024
        ),
    )(group_ids.T, expert_ids.T, gate_weights.T, tokens,
      *(jnp.swapaxes(w, 1, 2) for w in (gate_proj, up_proj, down_proj)))
    return pl.pallas_call(
        functools.partial(combine, n_dp),
        out_shape=jax.ShapeDtypeStruct((tok_rows, width), low),
        in_specs=[vmem, vmem],
        out_specs=vmem,
    )(parts, select)


def solution(mesh):
    placed = (
        P(("groups", "expert", "dp"), None),
        P(("groups", "expert", "dp"), None),
        P(("groups", "expert", "dp"), None),
        P(("groups", "expert", "dp"), None),
        P("expert", "dp", None),
        P("expert", "dp", None),
        P("expert", "dp", None),
    )
    return jax.shard_map(
        body,
        mesh=mesh,
        in_specs=placed,
        out_specs=P(("groups", "expert", "dp"), None),
        check_vma=False,
    )
```

```python
import functools

import jax
import jax.numpy as jnp
from jax import lax
from jax.experimental import pallas as pl
from jax.experimental.pallas import tpu as pltpu
from jax.sharding import PartitionSpec as P

GROUP_EXP = 3
SPAN = 4
CAP = 8
LANES = 128


def select_rows(group_ids, home, n_groups):
    tok_rows = group_ids.shape[1]
    n_rows = n_groups * CAP
    row = lax.broadcasted_iota(jnp.int32, (n_rows, tok_rows), 0)
    group = lax.rem(home + row // CAP, n_groups)
    member = jnp.zeros((n_rows, tok_rows), jnp.float32)
    for j in range(group_ids.shape[0]):
        member += (group_ids[j : j + 1, :] == group).astype(jnp.float32)
    first = lax.broadcasted_iota(jnp.int32, (tok_rows, tok_rows), 0)
    second = lax.broadcasted_iota(jnp.int32, (tok_rows, tok_rows), 1)
    earlier = (first < second).astype(jnp.bfloat16)
    rank = jnp.dot(member.astype(jnp.bfloat16), earlier, preferred_element_type=jnp.float32)
    slot = (row % CAP).astype(jnp.float32)
    return jnp.where(rank == slot, member, 0.0)


def expert_weights(expert_ids, gate_weights, home, n_groups, lanes):
    tok_rows = expert_ids.shape[1]
    row = lax.broadcasted_iota(jnp.int32, (lanes, tok_rows), 0)
    group = lax.rem(home + row // GROUP_EXP, n_groups)
    expert = jnp.where(row < n_groups * GROUP_EXP, group * GROUP_EXP + row % GROUP_EXP, -1)
    total = jnp.zeros((lanes, tok_rows), jnp.float32)
    for j in range(expert_ids.shape[0]):
        total += jnp.where(expert_ids[j : j + 1, :] == expert, gate_weights[j : j + 1, :], 0.0)
    return total


def kernel(
    n_groups, n_dp,
    gid_ref, eid_ref, gw_ref, tok_hbm, wg_hbm, wu_hbm, wd_hbm, out_ref, select_ref,
    tok, wg, wu, wd, sbuf, abuf, summed, final, near_bufs, far_bufs,
    lsem, own_sem, a_send, a_recv, b_send, b_recv, p_send, p_recv, h_send, h_recv,
    q_send, q_recv, c_send, c_recv,
):
    place = lax.axis_index("expert")
    core = lax.axis_index("dp")
    home = place // SPAN
    spot = place % SPAN
    half = tok.shape[1] // n_dp
    lanes = sbuf.shape[3] - half
    cols = wg.shape[0]
    wide = cols // GROUP_EXP

    loads = [
        pltpu.make_async_copy(src, dst, lsem.at[i])
        for i, (src, dst) in enumerate(
            [(tok_hbm, tok), (wg_hbm.at[0], wg), (wu_hbm.at[0], wu), (wd_hbm.at[0], wd)]
        )
    ]
    for load in loads:
        load.start()

    def member(dm, dd):
        return {"expert": home * SPAN + lax.rem(spot + dm, SPAN), "dp": lax.rem(core + dd, n_dp)}

    def group_peer(r):
        return {"expert": lax.rem(home + r, n_groups) * SPAN + spot, "dp": core}

    others = [(dm, dd) for dd in range(n_dp) for dm in range(SPAN) if (dm, dd) != (0, 0)]
    barrier = pltpu.get_barrier_semaphore()
    for r in range(1, n_groups):
        pl.semaphore_signal(barrier, inc=1, device_id=group_peer(r))
    for dm, dd in others:
        pl.semaphore_signal(barrier, inc=1, device_id=member(dm, dd))

    select = select_rows(gid_ref[...], home, n_groups)
    select_low = select.astype(jnp.bfloat16)
    select_ref[...] = select_low
    weights = expert_weights(
        eid_ref[...], gw_ref[...].astype(jnp.float32), home, n_groups, lanes
    ).astype(jnp.bfloat16)
    factor = lax.dot_general(
        select_low, weights, (((1,), (1,)), ((), ())), preferred_element_type=jnp.float32
    )
    factor = factor.reshape(n_groups, CAP, lanes).astype(jnp.bfloat16)
    loads[0].wait()
    for h in range(n_dp):
        picked = jnp.dot(
            select_low, tok[:, h * half : (h + 1) * half], preferred_element_type=jnp.float32
        )
        sbuf[h, :, :, :half] = picked.reshape(n_groups, CAP, half).astype(jnp.bfloat16)
        sbuf[h, :, :, half:] = factor
    pl.semaphore_wait(barrier, n_groups - 1 + len(others))

    def remote(src, dst, send, recv, device):
        return pltpu.make_async_remote_copy(
            src_ref=src, dst_ref=dst, send_sem=send, recv_sem=recv,
            device_id=device, device_id_type=pl.DeviceIdType.MESH,
        )

    others.sort(key=lambda pair: pair[1])
    n_far = n_groups - 1

    def turn(dd):
        return lax.rem(core + dd, n_dp)

    to_groups = {}
    for dd in range(n_dp):
        for r in range(1, n_groups):
            to_groups[dd, r] = remote(
                sbuf.at[turn(dd), r], abuf.at[turn(dd), r - 1],
                a_send.at[dd, r - 1], a_recv.at[dd, r - 1], group_peer(r),
            )
            to_groups[dd, r].start()

    other_core = member(0, 1)
    started = list(to_groups.values())

    def begin(*args):
        copy = remote(*args)
        copy.start()
        started.append(copy)
        return copy

    def chunked(total, step, work):
        if total <= step:
            work(0, total)
        else:

            @pl.loop(0, total // step)
            def _(i):
                work(i * step, step)

    def spread(n, dd, rows):
        src = sbuf.at[turn(dd), pl.ds(0, 1)] if n == 0 else abuf.at[turn(dd)]
        copies = []
        if dd == 0:
            own = pltpu.make_async_copy(src, rows.at[0, 0], own_sem.at[n])
            own.start()
            copies.append(own)
        for dm in range(SPAN):
            if (dm, dd) != (0, 0):
                spot_at = dd * SPAN + dm
                copies.append(
                    begin(
                        src, rows.at[dd, dm], b_send.at[n, spot_at], b_recv.at[n, spot_at],
                        member(dm, dd),
                    )
                )
        return copies

    def settle(copies):
        for copy in copies:
            if copy.is_remote:
                copy.wait_recv()
            else:
                copy.wait()

    def work_on(n, first_group, count, bufs):
        rows, part, got_part, hid, back, shares = bufs
        n_units = n_dp * SPAN * count
        half_units = n_units // n_dp
        half_rows = half_units * CAP
        units = rows.reshape(n_units, CAP, half + lanes)
        back_units = back.reshape(n_units, CAP, half)
        exchange = []
        for which, w in ((0, wg), (1, wu)):

            def project(start, size, which=which, w=w):
                block = units[pl.ds(start, size), :, :half].astype(jnp.float32)
                block = block.reshape(size * CAP, half).astype(jnp.bfloat16)
                part[which, pl.ds(pl.multiple_of(start * CAP, CAP), size * CAP), :] = (
                    lax.dot_general(
                        block, w[...], (((1,), (1,)), ((), ())),
                        preferred_element_type=jnp.float32,
                    )
                )

            chunked(n_units, n_dp * SPAN, project)
            exchange.append(
                begin(
                    part.at[which, pl.ds(half_rows, half_rows)], got_part.at[which],
                    p_send.at[n, which], p_recv.at[n, which], other_core,
                )
            )
        settle(exchange)

        def activate(start, size):
            total = size * CAP
            at = pl.ds(pl.multiple_of(start * CAP, CAP), total)
            gate_h = part[0, at, :] + got_part[0, at, :]
            up_h = part[1, at, :] + got_part[1, at, :]
            weight = units[pl.ds(start, size), :, half:].astype(jnp.float32)
            weight = weight.reshape(total, lanes)
            row = lax.broadcasted_iota(jnp.int32, (total, lanes), 0) + start * CAP
            lane = lax.broadcasted_iota(jnp.int32, (total, lanes), 1)
            first = (first_group + row // CAP % count) * GROUP_EXP
            col = lax.broadcasted_iota(jnp.int32, (total, cols), 1)
            scale = jnp.zeros((total, cols), jnp.float32)
            for k in range(GROUP_EXP):
                one = jnp.sum(jnp.where(lane == first + k, weight, 0.0), axis=1, keepdims=True)
                scale = jnp.where(col // wide == k, one, scale)
            active = gate_h / (1.0 + jnp.exp(-gate_h)) * up_h
            hid[0, at, :] = (active * scale).astype(jnp.bfloat16)

        chunked(half_units, SPAN, activate)
        hidden_copy = begin(hid.at[0], hid.at[1], h_send.at[n], h_recv.at[n], other_core)

        def lower(which):
            def work(start, size):
                at = pl.ds(pl.multiple_of(start * CAP, CAP), size * CAP)
                value = jnp.dot(hid[which, at, :], wd[...], preferred_element_type=jnp.float32)
                back_units[pl.ds(start + which * half_units, size)] = value.reshape(
                    size, CAP, half
                ).astype(jnp.bfloat16)

            chunked(half_units, SPAN, work)

        returns = {}
        for dd in range(n_dp):
            if dd == 1:
                settle([hidden_copy])
            lower(dd)
            for dm in range(SPAN):
                if (dm, dd) != (0, 0):
                    spot_at = dd * SPAN + dm
                    returns[dm, dd] = begin(
                        back.at[dd, dm], shares.at[dd, dm],
                        q_send.at[n, spot_at], q_recv.at[n, spot_at],
                        member(SPAN - dm, n_dp - dd),
                    )
        return returns

    def reduce(dd, bufs, returns):
        settle([returns[dm, dd] for dm in range(SPAN) if (dm, dd) in returns])
        total = None
        for dm in range(SPAN):
            src = bufs[4] if (dm, dd) == (0, 0) else bufs[5]
            value = src[dd, dm].astype(jnp.float32)
            total = value if total is None else total + value
        return total.astype(jnp.bfloat16)

    near_copies = spread(0, 0, near_bufs[0]) + spread(0, 1, near_bufs[0])
    far_copies = []
    for dd in range(n_dp):
        settle([to_groups[dd, r] for r in range(1, n_groups)])
        far_copies += spread(1, dd, far_bufs[0])
    for load in loads[1:]:
        load.wait()
    settle(near_copies)
    near_returns = work_on(0, 0, 1, near_bufs)
    settle(far_copies)
    far_returns = work_on(1, 1, n_far, far_bufs)
    for dd in range(n_dp):
        final[dd, pl.ds(0, 1)] = reduce(dd, near_bufs, near_returns)
    homeward = []
    for dd in range(n_dp):
        summed[dd] = reduce(dd, far_bufs, far_returns)
        for r in range(1, n_groups):
            homeward.append(
                begin(
                    summed.at[dd, r - 1], final.at[dd, r], c_send.at[dd, r - 1],
                    c_recv.at[dd, r - 1], group_peer(n_groups - r),
                )
            )
    for dd in range(n_dp):
        settle(homeward[dd * n_far : (dd + 1) * n_far])
        at = pl.multiple_of(turn(dd) * half, LANES)
        block = final[dd].astype(jnp.float32).reshape(n_groups * CAP, half)
        out_ref[:, pl.ds(at, half)] = block.astype(jnp.bfloat16)
    for copy in started:
        copy.wait_send()


def body(tokens, group_ids, expert_ids, gate_weights, gate_proj, up_proj, down_proj):
    tok_rows, width = tokens.shape
    n_groups = lax.axis_size("expert") // SPAN
    n_dp = lax.axis_size("dp")
    half = gate_proj.shape[1]
    cols = gate_proj.shape[2]
    lanes = -(-n_groups * GROUP_EXP // LANES) * LANES
    low, full = jnp.bfloat16, jnp.float32
    vmem = pl.BlockSpec(memory_space=pltpu.VMEM)
    hbm = pl.BlockSpec(memory_space=pl.ANY)
    dma = pltpu.SemaphoreType.DMA
    spots = n_dp * SPAN

    def buffers(count):
        n_rows = n_dp * SPAN * count * CAP
        return (
            pltpu.VMEM((n_dp, SPAN, count, CAP, half + lanes), low),
            pltpu.VMEM((2, n_rows, cols), full),
            pltpu.VMEM((2, n_rows // n_dp, cols), full),
            pltpu.VMEM((n_dp, n_rows // n_dp, cols), low),
            pltpu.VMEM((n_dp, SPAN, count, CAP, half), low),
            pltpu.VMEM((n_dp, SPAN, count, CAP, half), low),
        )

    parts, select = pl.pallas_call(
        functools.partial(kernel, n_groups, n_dp),
        out_shape=(
            jax.ShapeDtypeStruct((n_groups * CAP, width), low),
            jax.ShapeDtypeStruct((n_groups * CAP, tok_rows), low),
        ),
        in_specs=[vmem, vmem, vmem, hbm, hbm, hbm, hbm],
        out_specs=(vmem, vmem),
        scratch_shapes=[
            pltpu.VMEM((tok_rows, width), low),
            pltpu.VMEM((cols, half), low),
            pltpu.VMEM((cols, half), low),
            pltpu.VMEM((cols, half), low),
            pltpu.VMEM((n_dp, n_groups, CAP, half + lanes), low),
            pltpu.VMEM((n_dp, n_groups - 1, CAP, half + lanes), low),
            pltpu.VMEM((n_dp, n_groups - 1, CAP, half), low),
            pltpu.VMEM((n_dp, n_groups, CAP, half), low),
            buffers(1),
            buffers(n_groups - 1),
            dma((4,)), dma((2,)),
            dma((n_dp, n_groups - 1)), dma((n_dp, n_groups - 1)),
            dma((2, spots)), dma((2, spots)),
            dma((2, 2)), dma((2, 2)), dma((2,)), dma((2,)),
            dma((2, spots)), dma((2, spots)),
            dma((n_dp, n_groups - 1)), dma((n_dp, n_groups - 1)),
        ],
        compiler_params=pltpu.CompilerParams(
            collective_id=0, has_side_effects=True, vmem_limit_bytes=60 * 1024 * 1024
        ),
    )(group_ids.T, expert_ids.T, gate_weights.T, tokens,
      *(jnp.swapaxes(w, 1, 2) for w in (gate_proj, up_proj, down_proj)))
    result = lax.dot_general(
        select, parts, (((0,), (0,)), ((), ())), preferred_element_type=jnp.float32
    )
    return result.astype(low)


def solution(mesh):
    placed = (
        P(("groups", "expert", "dp"), None),
        P(("groups", "expert", "dp"), None),
        P(("groups", "expert", "dp"), None),
        P(("groups", "expert", "dp"), None),
        P("expert", "dp", None),
        P("expert", "dp", None),
        P("expert", "dp", None),
    )
    return jax.shard_map(
        body,
        mesh=mesh,
        in_specs=placed,
        out_specs=P(("groups", "expert", "dp"), None),
        check_vma=False,
    )
```

```python
import functools

import jax
import jax.numpy as jnp
from jax import lax
from jax.experimental import pallas as pl
from jax.experimental.pallas import tpu as pltpu
from jax.sharding import PartitionSpec as P

GROUP_EXP = 3
SPAN = 4
CAP = 8
LANES = 128


def select_rows(group_ids, home, n_groups):
    tok_rows = group_ids.shape[1]
    n_rows = n_groups * CAP
    row = lax.broadcasted_iota(jnp.int32, (n_rows, tok_rows), 0)
    group = lax.rem(home + row // CAP, n_groups)
    member = jnp.zeros((n_rows, tok_rows), jnp.float32)
    for j in range(group_ids.shape[0]):
        member += (group_ids[j : j + 1, :] == group).astype(jnp.float32)
    first = lax.broadcasted_iota(jnp.int32, (tok_rows, tok_rows), 0)
    second = lax.broadcasted_iota(jnp.int32, (tok_rows, tok_rows), 1)
    earlier = (first < second).astype(jnp.bfloat16)
    rank = jnp.dot(member.astype(jnp.bfloat16), earlier, preferred_element_type=jnp.float32)
    slot = (row % CAP).astype(jnp.float32)
    return jnp.where(rank == slot, member, 0.0)


def expert_weights(expert_ids, gate_weights, home, n_groups, lanes):
    tok_rows = expert_ids.shape[1]
    row = lax.broadcasted_iota(jnp.int32, (lanes, tok_rows), 0)
    group = lax.rem(home + row // GROUP_EXP, n_groups)
    expert = jnp.where(row < n_groups * GROUP_EXP, group * GROUP_EXP + row % GROUP_EXP, -1)
    total = jnp.zeros((lanes, tok_rows), jnp.float32)
    for j in range(expert_ids.shape[0]):
        total += jnp.where(expert_ids[j : j + 1, :] == expert, gate_weights[j : j + 1, :], 0.0)
    return total


def kernel(
    n_groups, n_dp,
    gid_ref, eid_ref, gw_ref, tok_hbm, wg_hbm, wu_hbm, wd_hbm, out_ref, select_ref,
    tok, wg, wu, wd, sbuf, abuf, summed, final, near_bufs, far_bufs,
    lsem, own_sem, a_send, a_recv, b_send, b_recv, w_send, w_recv,
    q_send, q_recv, c_send, c_recv,
):
    place = lax.axis_index("expert")
    core = lax.axis_index("dp")
    home = place // SPAN
    spot = place % SPAN
    half = tok.shape[1] // n_dp
    width = tok.shape[1]
    lanes = sbuf.shape[2] - width
    cols = wg.shape[1]
    wide = cols // GROUP_EXP

    loads = [
        pltpu.make_async_copy(src, dst, lsem.at[i])
        for i, (src, dst) in enumerate(
            [
                (tok_hbm, tok), (wg_hbm.at[0], wg.at[core]), (wu_hbm.at[0], wu.at[core]),
                (wd_hbm.at[0], wd.at[core]),
            ]
        )
    ]
    for load in loads:
        load.start()

    def member(dm, dd):
        return {"expert": home * SPAN + lax.rem(spot + dm, SPAN), "dp": lax.rem(core + dd, n_dp)}

    def group_peer(r):
        return {"expert": lax.rem(home + r, n_groups) * SPAN + spot, "dp": core}

    others = [(dm, 0) for dm in range(1, SPAN)] + [(0, dd) for dd in range(1, n_dp)]
    barrier = pltpu.get_barrier_semaphore()
    for r in range(1, n_groups):
        pl.semaphore_signal(barrier, inc=1, device_id=group_peer(r))
    for dm, dd in others:
        pl.semaphore_signal(barrier, inc=1, device_id=member(dm, dd))

    select = select_rows(gid_ref[...], home, n_groups)
    select_low = select.astype(jnp.bfloat16)
    select_ref[...] = select_low
    weights = expert_weights(
        eid_ref[...], gw_ref[...].astype(jnp.float32), home, n_groups, lanes
    ).astype(jnp.bfloat16)
    factor = lax.dot_general(
        select_low, weights, (((1,), (1,)), ((), ())), preferred_element_type=jnp.float32
    )
    factor = factor.reshape(n_groups, CAP, lanes).astype(jnp.bfloat16)
    loads[0].wait()
    picked = jnp.dot(select_low, tok[...], preferred_element_type=jnp.float32)
    sbuf[:, :, :width] = picked.reshape(n_groups, CAP, width).astype(jnp.bfloat16)
    sbuf[:, :, width:] = factor
    pl.semaphore_wait(barrier, n_groups - 1 + len(others))

    def remote(src, dst, send, recv, device):
        return pltpu.make_async_remote_copy(
            src_ref=src, dst_ref=dst, send_sem=send, recv_sem=recv,
            device_id=device, device_id_type=pl.DeviceIdType.MESH,
        )

    n_far = n_groups - 1
    started = []

    def begin(*args):
        copy = remote(*args)
        copy.start()
        started.append(copy)
        return copy

    pieces = [pl.ds(0, half), pl.ds(half, width - half + lanes)]
    to_groups = {}
    for p, piece in enumerate(pieces):
        for r in range(1, n_groups):
            to_groups[p, r] = begin(
                sbuf.at[r, :, piece], abuf.at[r - 1, :, piece],
                a_send.at[p, r - 1], a_recv.at[p, r - 1], group_peer(r),
            )

    def chunked(total, step, work):
        if total <= step:
            work(0, total)
        else:

            @pl.loop(0, total // step)
            def _(i):
                work(i * step, step)

    def spread(n, p, rows):
        src = sbuf.at[pl.ds(0, 1), :, pieces[p]] if n == 0 else abuf.at[:, :, pieces[p]]
        own = pltpu.make_async_copy(src, rows.at[0, :, :, pieces[p]], own_sem.at[n, p])
        own.start()
        copies = [own]
        for dm in range(1, SPAN):
            copies.append(
                begin(
                    src, rows.at[dm, :, :, pieces[p]], b_send.at[n, p * SPAN + dm],
                    b_recv.at[n, p * SPAN + dm], member(dm, 0),
                )
            )
        return copies

    def settle(copies):
        for copy in copies:
            if copy.is_remote:
                copy.wait_recv()
            else:
                copy.wait()

    def work_on(n, first_group, count, bufs):
        rows, part, hid, back, shares = bufs
        n_units = SPAN * count
        units = rows.reshape(n_units, CAP, width + lanes)
        back_units = back.reshape(n_dp, n_units, CAP, half)

        def project(start, size):
            block = units[pl.ds(start, size), :, :width].astype(jnp.float32)
            block = block.reshape(size * CAP, width).astype(jnp.bfloat16)
            for which, w in ((0, wg), (1, wu)):
                total = None
                for h in range(n_dp):
                    value = lax.dot_general(
                        block[:, h * half : (h + 1) * half], w[h], (((1,), (1,)), ((), ())),
                        preferred_element_type=jnp.float32,
                    )
                    total = value if total is None else total + value
                at = pl.ds(pl.multiple_of(start * CAP, CAP), size * CAP)
                part[which, at, :] = total

        chunked(n_units, SPAN, project)

        def activate(start, size):
            total = size * CAP
            at = pl.ds(pl.multiple_of(start * CAP, CAP), total)
            gate_h = part[0, at, :]
            up_h = part[1, at, :]
            weight = units[pl.ds(start, size), :, width:].astype(jnp.float32)
            weight = weight.reshape(total, lanes)
            row = lax.broadcasted_iota(jnp.int32, (total, lanes), 0) + start * CAP
            lane = lax.broadcasted_iota(jnp.int32, (total, lanes), 1)
            first = (first_group + row // CAP % count) * GROUP_EXP
            col = lax.broadcasted_iota(jnp.int32, (total, cols), 1)
            scale = jnp.zeros((total, cols), jnp.float32)
            for k in range(GROUP_EXP):
                one = jnp.sum(jnp.where(lane == first + k, weight, 0.0), axis=1, keepdims=True)
                scale = jnp.where(col // wide == k, one, scale)
            active = gate_h / (1.0 + jnp.exp(-gate_h)) * up_h
            hid[at, :] = (active * scale).astype(jnp.bfloat16)

        chunked(n_units, SPAN, activate)
        returns = {}
        for h in range(n_dp):

            def lower(start, size, h=h):
                at = pl.ds(pl.multiple_of(start * CAP, CAP), size * CAP)
                value = jnp.dot(hid[at, :], wd[h], preferred_element_type=jnp.float32)
                back_units[h, pl.ds(start, size)] = value.reshape(size, CAP, half).astype(
                    jnp.bfloat16
                )

            chunked(n_units, SPAN, lower)
            for dm in range(1, SPAN):
                returns[dm, h] = begin(
                    back.at[h, dm], shares.at[h, dm], q_send.at[n, h * SPAN + dm],
                    q_recv.at[n, h * SPAN + dm], member(SPAN - dm, 0),
                )
        return returns

    def reduce(dd, bufs, returns):
        settle([returns[dm, dd] for dm in range(SPAN) if (dm, dd) in returns])
        total = None
        for dm in range(SPAN):
            src = bufs[3] if dm == 0 else bufs[4]
            value = src[dd, dm].astype(jnp.float32)
            total = value if total is None else total + value
        return total.astype(jnp.bfloat16)

    swaps = []
    near_copies = spread(0, 0, near_bufs[0]) + spread(0, 1, near_bufs[0])
    for i, (src, dst) in enumerate(((wg_hbm, wg), (wu_hbm, wu), (wd_hbm, wd))):
        for dd in range(1, n_dp):
            swaps.append(
                begin(src.at[0], dst.at[core], w_send.at[i], w_recv.at[i], member(0, dd))
            )
    far_copies = []
    for dd in range(n_dp):
        settle([to_groups[dd, r] for r in range(1, n_groups)])
        far_copies += spread(1, dd, far_bufs[0])
    for load in loads[1:]:
        load.wait()
    settle(swaps + near_copies)
    near_returns = work_on(0, 0, 1, near_bufs)
    settle(far_copies)
    far_returns = work_on(1, 1, n_far, far_bufs)
    for dd in range(n_dp):
        final[dd, pl.ds(0, 1)] = reduce(dd, near_bufs, near_returns)
    homeward = []
    for dd in range(n_dp):
        summed[dd] = reduce(dd, far_bufs, far_returns)
        for r in range(1, n_groups):
            homeward.append(
                begin(
                    summed.at[dd, r - 1], final.at[dd, r], c_send.at[dd, r - 1],
                    c_recv.at[dd, r - 1], group_peer(n_groups - r),
                )
            )
    for dd in range(n_dp):
        settle(homeward[dd * n_far : (dd + 1) * n_far])
        at = dd * half
        block = final[dd].astype(jnp.float32).reshape(n_groups * CAP, half)
        out_ref[:, at : at + half] = block.astype(jnp.bfloat16)
    for copy in started:
        copy.wait_send()


def body(tokens, group_ids, expert_ids, gate_weights, gate_proj, up_proj, down_proj):
    tok_rows, width = tokens.shape
    n_groups = lax.axis_size("expert") // SPAN
    n_dp = lax.axis_size("dp")
    half = gate_proj.shape[1]
    cols = gate_proj.shape[2]
    lanes = -(-n_groups * GROUP_EXP // LANES) * LANES
    low, full = jnp.bfloat16, jnp.float32
    vmem = pl.BlockSpec(memory_space=pltpu.VMEM)
    hbm = pl.BlockSpec(memory_space=pl.ANY)
    dma = pltpu.SemaphoreType.DMA
    spots = n_dp * SPAN

    def buffers(count):
        n_rows = SPAN * count * CAP
        return (
            pltpu.VMEM((SPAN, count, CAP, width + lanes), low),
            pltpu.VMEM((2, n_rows, cols), full),
            pltpu.VMEM((n_rows, cols), low),
            pltpu.VMEM((n_dp, SPAN, count, CAP, half), low),
            pltpu.VMEM((n_dp, SPAN, count, CAP, half), low),
        )

    parts, select = pl.pallas_call(
        functools.partial(kernel, n_groups, n_dp),
        out_shape=(
            jax.ShapeDtypeStruct((n_groups * CAP, width), low),
            jax.ShapeDtypeStruct((n_groups * CAP, tok_rows), low),
        ),
        in_specs=[vmem, vmem, vmem, hbm, hbm, hbm, hbm],
        out_specs=(vmem, vmem),
        scratch_shapes=[
            pltpu.VMEM((tok_rows, width), low),
            pltpu.VMEM((n_dp, cols, half), low),
            pltpu.VMEM((n_dp, cols, half), low),
            pltpu.VMEM((n_dp, cols, half), low),
            pltpu.VMEM((n_groups, CAP, width + lanes), low),
            pltpu.VMEM((n_groups - 1, CAP, width + lanes), low),
            pltpu.VMEM((n_dp, n_groups - 1, CAP, half), low),
            pltpu.VMEM((n_dp, n_groups, CAP, half), low),
            buffers(1),
            buffers(n_groups - 1),
            dma((4,)), dma((2, 2)),
            dma((n_dp, n_groups - 1)), dma((n_dp, n_groups - 1)),
            dma((2, spots)), dma((2, spots)),
            dma((3,)), dma((3,)),
            dma((2, spots)), dma((2, spots)),
            dma((n_dp, n_groups - 1)), dma((n_dp, n_groups - 1)),
        ],
        compiler_params=pltpu.CompilerParams(
            collective_id=0, has_side_effects=True, vmem_limit_bytes=60 * 1024 * 1024
        ),
    )(group_ids.T, expert_ids.T, gate_weights.T, tokens,
      *(jnp.swapaxes(w, 1, 2) for w in (gate_proj, up_proj, down_proj)))
    result = lax.dot_general(
        select, parts, (((0,), (0,)), ((), ())), preferred_element_type=jnp.float32
    )
    return result.astype(low)


def solution(mesh):
    placed = (
        P(("groups", "expert", "dp"), None),
        P(("groups", "expert", "dp"), None),
        P(("groups", "expert", "dp"), None),
        P(("groups", "expert", "dp"), None),
        P("expert", "dp", None),
        P("expert", "dp", None),
        P("expert", "dp", None),
    )
    return jax.shard_map(
        body,
        mesh=mesh,
        in_specs=placed,
        out_specs=P(("groups", "expert", "dp"), None),
        check_vma=False,
    )
```
